256 devices in a mesh: grp: 8 (over z), mem: 32 (over y, x, core).
Axes of the slice: x: 4, y: 4, z: 8, core: 2. Of those that a mesh axis runs over, the one named last changes fastest.
Arguments:
- child_means: float32 [524288, 64], P(('grp', 'mem')), may hold values from -48 to 48
- child_variances: float32 [524288, 64], P(('grp', 'mem')), may hold values from 0.2 to 2
- virtual_counts: int32 [524288], P(('grp', 'mem')), may hold values from 1 to 4
- assignment: int32 [524288, 1], P(('grp', 'mem')), may hold values from 0 to 511
Outputs:
- parent_means: float32 [512, 64], P('mem')
- parent_variances: float32 [512, 64], P('mem')
- parent_weights: float32 [512], P('mem')
The draws below stay inside these ranges and needn't reach their ends.
All inputs are finite; a program needn't handle non-finite values.
Results may differ from the reference program's by a relative error of at most 0.0003.
Values sent between devices are 32-bit elements; how exact they have to be, the bound alone decides.
No kernel may reach another device: no remote copies, remote signals or barrier semaphores. Data moves between devices by JAX's collectives and lax.ppermute only.
A program may use at most 64 MiB of HBM per device.

```python
import math
import jax
import jax.numpy as jnp
from jax import lax

D = 64
P_SIZE = 512
ITERS = 2
CHILDREN = 524288


def draw_child_means(key, part):
    return jnp.clip(jax.random.normal(key, (CHILDREN, D), jnp.float32), -6.0, 6.0)


def touch_ends(drawn, key, low, high):
    longest = drawn.shape.index(max(drawn.shape))
    spots = []
    for shift in (0, 1):
        where = [jax.random.randint(jax.random.fold_in(key, axis), (), 0, length) for axis, length in enumerate(drawn.shape)]
        where[longest] = (where[longest] + shift) % drawn.shape[longest]
        spots.append(tuple(where))
    return drawn.at[spots[0]].set(low).at[spots[1]].set(high)


def level_of(stream_key, dims, cuts, least, high):
    gain, own = 1.0, jax.random.fold_in(stream_key, 6)
    for dim, blocks in cuts:
        draws = jnp.exp(jax.random.uniform(jax.random.fold_in(own, dim), (blocks,), jnp.float32, least / len(cuts), high / len(cuts)))
        gain = gain * jnp.repeat(draws, dims[dim] // blocks).reshape([-1 if axis == dim else 1 for axis in range(len(dims))])
    return gain


def distinct(own_key, rows, amount, top, lift):
    ranking = jax.random.permutation(jax.random.fold_in(own_key, 1), amount)
    favour = ranking
    for power in range(3):
        favour = favour * favour // amount
    favour = favour * lift // amount
    lots = jax.random.randint(jax.random.fold_in(own_key, 2), (rows, amount), 0, 4096) + favour
    fixed_rows = jax.random.permutation(jax.random.fold_in(own_key, 3), rows)[jnp.arange(amount) % rows]
    lots = jnp.where(jnp.arange(rows)[:, None] == fixed_rows[None, :], 1 << 14, lots)
    priority = lots * amount + jnp.arange(amount)
    return lax.top_k(priority.astype(jnp.int32), top)[1].astype(jnp.int32)


def setup_inputs(seed: int = 0) -> dict:
    streams_of = jax.random.split(jax.random.key(seed), 5)
    return {
        "child_means": draw_child_means(jax.random.fold_in(streams_of[4], 71), 0),
        "child_variances": jnp.clip(jnp.exp(math.log(2.0) - 2.3025851 * jax.random.uniform(streams_of[1], (CHILDREN, D), jnp.float32) ** level_of(streams_of[1], (CHILDREN, D), ((0, 256),), -0.2, 0.2)), 0.2, 2.0),
        "virtual_counts": touch_ends(jax.random.randint(streams_of[2], (CHILDREN,), 1, 5), jax.random.fold_in(streams_of[2], 1), 1, 4).astype(jnp.int32),
        "assignment": distinct(streams_of[3], CHILDREN, P_SIZE, 1, 0),
    }


def child_features(means, variances):
    return jnp.concatenate([means, variances + means * means], axis=1)


def accumulate(features, extras, weigh):
    row_count = features.shape[0]
    block = math.gcd(row_count, 1024)
    turns = row_count // block
    pieces = (features.reshape(turns, block, features.shape[1]),) + tuple(
        extra.reshape((turns, block) + extra.shape[1:]) for extra in extras)

    def advance(carry, piece):
        weights = weigh(*piece)
        sums = carry[0] + lax.dot_general(weights, piece[0], (((0,), (0,)), ((), ())),
                                          precision=lax.Precision.HIGHEST,
                                          preferred_element_type=jnp.float32)
        counts = carry[1] + jnp.sum(weights, axis=0)
        return (sums, counts), None

    start_sums = (jnp.zeros((P_SIZE, features.shape[1]), jnp.float32), jnp.zeros((P_SIZE,), jnp.float32))
    return lax.scan(advance, start_sums, pieces)[0]


def maximize(counts, sums, total):
    width = sums.shape[1] // 2
    mass = counts + 1.0
    means = sums[:, :width] / mass[:, None]
    second = (sums[:, width:] + 1.0) / mass[:, None]
    return means, second - means * means, mass / (total + P_SIZE)


def parent_table(means, variances, weights):
    inverse = 1.0 / variances
    table = jnp.concatenate([-2.0 * means * inverse, inverse], axis=1)
    offset = jnp.sum(jnp.log(2.0 * math.pi * variances) + means * means * inverse, axis=1)
    return table, offset, jnp.log(weights)


def soft_weights(block_features, block_virtual, table, offset, log_weight):
    width = block_features.shape[1] // 2
    cross = lax.dot_general(block_features, table, (((1,), (1,)), ((), ())),
                            precision=lax.Precision.HIGHEST, preferred_element_type=jnp.float32)
    ell = (-0.5 / width) * (cross + offset[None, :])
    score = log_weight[None, :] + block_virtual[:, None] * ell
    top = jnp.max(score, axis=1, keepdims=True)
    expd = jnp.exp(score - top)
    resp = expd / jnp.sum(expd, axis=1, keepdims=True)
    return resp * block_virtual[:, None]


def reference(child_means, child_variances, virtual_counts, assignment):
    features = child_features(child_means, child_variances)
    virtual = virtual_counts.astype(jnp.float32)
    total = jnp.sum(virtual)
    labels = jnp.arange(P_SIZE, dtype=jnp.int32)

    def initial_weights(block_features, block_virtual, block_assign):
        return (block_assign[:, 0:1] == labels[None, :]).astype(jnp.float32) * block_virtual[:, None]

    sums, counts = accumulate(features, (virtual, assignment), initial_weights)
    means, variances, weights = maximize(counts, sums, total)
    for iteration in range(ITERS):
        table, offset, log_weight = parent_table(means, variances, weights)

        def weigh(block_features, block_virtual):
            return soft_weights(block_features, block_virtual, table, offset, log_weight)

        sums, counts = accumulate(features, (virtual,), weigh)
        means, variances, weights = maximize(counts, sums, total)
    return means, variances, weights
```

```python
import math

import jax
import jax.numpy as jnp
from jax import lax
from jax.experimental import pallas as pl
from jax.experimental.pallas import tpu as pltpu
from jax.sharding import Mesh
from jax.sharding import PartitionSpec as P

D = 64
P_SIZE = 512
ITERS = 2
MEM_SIZE = 32
OWN = P_SIZE // MEM_SIZE
PIECE = OWN + 1
TILE = 256
GRP_MEM = ("grp", "mem_0", "mem_1", "mem_2")
MEM = ("mem_0", "mem_1", "mem_2")
LOG2E = math.log2(math.e)


def in_two(value):
    high = value.astype(jnp.bfloat16)
    return high, (value - high.astype(jnp.float32)).astype(jnp.bfloat16)


def write_pieces(sums, counts, local_total, out_ref):
    lane = lax.broadcasted_iota(jnp.int32, (OWN, 128), 1)
    row = lax.broadcasted_iota(jnp.int32, (OWN, 128), 0)
    last = lax.broadcasted_iota(jnp.int32, (1, 128), 1) == OWN
    for m in range(MEM_SIZE):
        own = slice(m * OWN, (m + 1) * OWN)
        out_ref[m * PIECE : m * PIECE + OWN, :] = sums[own]
        spread = jnp.where(lane == row, counts[own], 0.0)
        flat = jnp.sum(spread, axis=0, keepdims=True)
        out_ref[m * PIECE + OWN : (m + 1) * PIECE, :] = jnp.where(last, local_total, flat)


def first_kernel(mean_ref, var_ref, virt_ref, label_ref, feat_ref, out_ref, acc_ref, cnt_ref):
    n = mean_ref.shape[0]
    for t in range(n // TILE):
        rows = slice(t * TILE, (t + 1) * TILE)
        mean = mean_ref[rows, :]
        feats = jnp.concatenate([mean, var_ref[rows, :] + mean * mean], axis=1)
        high, low = in_two(feats)
        feat_ref[rows, :128] = high
        feat_ref[rows, 128:] = low
        parent = lax.broadcasted_iota(jnp.int32, (P_SIZE, TILE), 0)
        virt = virt_ref[:, rows].astype(jnp.float32)
        w = jnp.where(parent == label_ref[:, rows], virt, 0.0)
        part = jnp.dot(
            w.astype(jnp.bfloat16), feat_ref[rows, :], preferred_element_type=jnp.float32
        )
        seen = w[:, :128] + w[:, 128:]
        if t == 0:
            acc_ref[...] = part
            cnt_ref[...] = seen
        else:
            acc_ref[...] += part
            cnt_ref[...] += seen
    finish(virt_ref, acc_ref, cnt_ref, out_ref)


def finish(virt_ref, acc_ref, cnt_ref, out_ref):
    local_total = jnp.sum(virt_ref[...].astype(jnp.float32), axis=1, keepdims=True)
    counts = jnp.sum(cnt_ref[...], axis=1, keepdims=True)
    write_pieces(acc_ref[:, :128] + acc_ref[:, 128:], counts, local_total, out_ref)


def step_kernel(table_ref, feat_ref, virt_ref, out_ref, tab_ref, off_ref, score_ref, w_ref, acc_ref, cnt_ref):
    n = feat_ref.shape[0]
    lane = lax.broadcasted_iota(jnp.int32, (OWN, 128), 1)
    row = lax.broadcasted_iota(jnp.int32, (OWN, 128), 0)
    for m in range(MEM_SIZE):
        own = slice(m * OWN, (m + 1) * OWN)
        high, low = in_two(table_ref[m * PIECE : m * PIECE + OWN, :])
        tab_ref[own, 0:128] = high
        tab_ref[own, 128:256] = high
        tab_ref[own, 256:384] = low
        tab_ref[own, 384:512] = low
        extra = jnp.broadcast_to(table_ref[m * PIECE + OWN : (m + 1) * PIECE, :], (OWN, 128))
        for k in range(2):
            column = jnp.sum(jnp.where(lane == row + k * OWN, extra, 0.0), axis=1, keepdims=True)
            off_ref[own, k * 128 : (k + 1) * 128] = jnp.broadcast_to(column, (OWN, 128))
    for t in range(n // TILE):
        rows = slice(t * TILE, (t + 1) * TILE)
        slot = t % 2
        feats = feat_ref[rows, :]
        twice = jnp.concatenate([feats, feats], axis=1)
        cross = lax.dot_general(
            tab_ref[...], twice, (((1,), (1,)), ((), ())), preferred_element_type=jnp.float32
        )
        virt = virt_ref[:, rows].astype(jnp.float32)
        for h in range(TILE // 128):
            half = slice(h * 128, (h + 1) * 128)
            v = virt[:, half]
            score = (cross[:, half] + off_ref[:, :128]) * v + off_ref[:, 128:]
            score_ref[slot, :, half] = score
        score = score_ref[slot]
        top = jnp.max(score, axis=0, keepdims=True)
        expd = jnp.exp2(score - top)
        ratio = virt / jnp.sum(expd, axis=0, keepdims=True)
        w = expd * ratio
        high, low = in_two(w)
        w_ref[slot, :, :TILE] = high
        w_ref[slot, :, TILE:] = low
        part = jnp.dot(
            w_ref[slot], jnp.concatenate([feats, feats], axis=0), preferred_element_type=jnp.float32
        )
        seen = w[:, :128] + w[:, 128:]
        if t == 0:
            acc_ref[...] = part
            cnt_ref[...] = seen
        else:
            acc_ref[...] += part
            cnt_ref[...] += seen
    finish(virt_ref, acc_ref, cnt_ref, out_ref)


def vmem(k):
    return [pl.BlockSpec(memory_space=pltpu.VMEM)] * k


def first_statistics(means, variances, virt, labels, **kw):
    n = means.shape[0]
    return pl.pallas_call(
        first_kernel,
        out_shape=(
            jax.ShapeDtypeStruct((n, 256), jnp.bfloat16),
            jax.ShapeDtypeStruct((MEM_SIZE * PIECE, 128), jnp.float32),
        ),
        in_specs=vmem(4),
        out_specs=tuple(vmem(2)),
        scratch_shapes=[pltpu.VMEM((P_SIZE, 256), jnp.float32), pltpu.VMEM((P_SIZE, 128), jnp.float32)],
        name="first",
        **kw,
    )(means, variances, virt, labels)


def step_statistics(table, feats, virt, **kw):
    return pl.pallas_call(
        step_kernel,
        out_shape=jax.ShapeDtypeStruct((MEM_SIZE * PIECE, 128), jnp.float32),
        in_specs=vmem(3),
        out_specs=vmem(1)[0],
        scratch_shapes=[
            pltpu.VMEM((P_SIZE, 512), jnp.bfloat16),
            pltpu.VMEM((P_SIZE, 256), jnp.float32),
            pltpu.VMEM((2, P_SIZE, TILE), jnp.float32),
            pltpu.VMEM((2, P_SIZE, 2 * TILE), jnp.bfloat16),
            pltpu.VMEM((P_SIZE, 256), jnp.float32),
            pltpu.VMEM((P_SIZE, 128), jnp.float32),
        ],
        name="step",
        **kw,
    )(table, feats, virt)


def reduce_own(pieces):
    size = lax.axis_size("grp")
    arrived = lax.all_to_all(pieces.reshape(MEM_SIZE, 1, PIECE * 128), MEM, 0, 0, tiled=True)
    shared = jnp.sum(arrived, axis=0, keepdims=True)
    copies = lax.all_to_all(
        jnp.broadcast_to(shared, (size, 1, PIECE * 128)), "grp", 0, 0, tiled=True
    )
    return jnp.sum(copies, axis=(0, 1))


def maximize(own):
    sums = own[: OWN * 128].reshape(OWN, 128)
    mass = own[OWN * 128 : OWN * 128 + OWN] + 1.0
    total = own[OWN * 128 + OWN]
    means = sums[:, :D] / mass[:, None]
    second = (sums[:, D:] + 1.0) / mass[:, None]
    return means, second - means * means, mass / (total + P_SIZE)


def parent_table(means, variances, weights):
    scale = -0.5 / D * LOG2E
    inverse = scale / variances
    table = jnp.concatenate([-2.0 * means * inverse, inverse], axis=1)
    offset = jnp.sum(scale * jnp.log(2.0 * math.pi * variances) + means * means * inverse, axis=1)
    extra = jnp.concatenate([offset, LOG2E * jnp.log(weights), jnp.zeros((128 - 2 * OWN,), jnp.float32)])
    piece = jnp.concatenate([table.reshape(-1), extra])
    gathered = lax.all_to_all(
        jnp.broadcast_to(piece[None, None], (MEM_SIZE, 1, PIECE * 128)), MEM, 0, 0, tiled=True
    )
    return gathered.reshape(MEM_SIZE * PIECE, 128)


def shards(child_means, child_variances, virtual_counts, assignment):
    virt = virtual_counts.reshape(1, -1)
    feats, pieces = first_statistics(child_means, child_variances, virt, assignment.reshape(1, -1))
    means, variances, weights = maximize(reduce_own(pieces))
    for iteration in range(ITERS):
        table = parent_table(means, variances, weights)
        pieces = step_statistics(table, feats, virt)
        means, variances, weights = maximize(reduce_own(pieces))
    return (means, variances, weights)


def solution(mesh):
    split = Mesh(
        mesh.devices.reshape(mesh.shape["grp"], 4, 4, 2), ("grp", "mem_0", "mem_1", "mem_2")
    )
    return jax.shard_map(
        shards,
        mesh=split,
        in_specs=(P(GRP_MEM, None), P(GRP_MEM, None), P(GRP_MEM), P(GRP_MEM, None)),
        out_specs=(P(MEM, None), P(MEM, None), P(MEM)),
        check_vma=False,
    )
```

```python
import math

import jax
import jax.numpy as jnp
from jax import lax
from jax.experimental import pallas as pl
from jax.experimental.pallas import tpu as pltpu
from jax.sharding import Mesh
from jax.sharding import PartitionSpec as P

D = 64
P_SIZE = 512
ITERS = 2
MEM_SIZE = 32
OWN = P_SIZE // MEM_SIZE
PIECE = OWN + 1
TILE = 256
GRP_MEM = ("grp", "mem_0", "mem_1", "mem_2")
MEM = ("mem_0", "mem_1", "mem_2")
LOG2E = math.log2(math.e)
CONTRACT_LANES = (((1,), (1,)), ((), ()))


def in_two(value):
    high = value.astype(jnp.bfloat16)
    return high, (value - high.astype(jnp.float32)).astype(jnp.bfloat16)


def write_pieces(sums, counts, local_total, out_ref):
    lane = lax.broadcasted_iota(jnp.int32, (OWN, 128), 1)
    row = lax.broadcasted_iota(jnp.int32, (OWN, 128), 0)
    last = lax.broadcasted_iota(jnp.int32, (1, 128), 1) == OWN
    for m in range(MEM_SIZE):
        own = slice(m * OWN, (m + 1) * OWN)
        out_ref[m * PIECE : m * PIECE + OWN, :] = sums[own]
        spread = jnp.where(lane == row, counts[own], 0.0)
        flat = jnp.sum(spread, axis=0, keepdims=True)
        out_ref[m * PIECE + OWN : (m + 1) * PIECE, :] = jnp.where(last, local_total, flat)


def first_kernel(
    mean_hbm, var_hbm, virt_hbm, label_hbm, feat_ref, out_ref,
    mean_ref, var_ref, virt_ref, label_ref, acc_ref, cnt_ref, sem
):
    n = mean_ref.shape[1]
    copies = [
        pltpu.make_async_copy(source, target, sem.at[k])
        for k, (source, target) in enumerate(
            (
                (label_hbm, label_ref),
                (virt_hbm, virt_ref),
                (mean_hbm, mean_ref),
                (var_hbm, var_ref),
            )
        )
    ]
    for copy in copies:
        copy.start()
    for copy in copies[:2]:
        copy.wait()
    for t in range(n // TILE):
        rows = slice(t * TILE, (t + 1) * TILE)
        virt = virt_ref[:, rows].astype(jnp.float32)
        parent = lax.broadcasted_iota(jnp.int32, (P_SIZE, TILE), 0)
        w = jnp.where(parent == label_ref[:, rows], virt, 0.0)
        if t == 0:
            for copy in copies[2:]:
                copy.wait()
        mean = mean_ref[:, rows]
        high, low = in_two(jnp.concatenate([mean, var_ref[:, rows] + mean * mean], axis=0))
        feats = jnp.concatenate([high, low], axis=0)
        feat_ref[:, rows] = feats
        part = lax.dot_general(
            w.astype(jnp.bfloat16), feats, CONTRACT_LANES, preferred_element_type=jnp.float32
        )
        add_up(t, part, w, acc_ref, cnt_ref)
    finish(virt_ref, acc_ref, cnt_ref, out_ref)


def add_up(t, part, w, acc_ref, cnt_ref):
    seen = w[:, :128] + w[:, 128:]
    if t == 0:
        acc_ref[...] = part
        cnt_ref[...] = seen
    else:
        acc_ref[...] += part
        cnt_ref[...] += seen


def finish(virt_ref, acc_ref, cnt_ref, out_ref):
    local_total = jnp.sum(virt_ref[...].astype(jnp.float32), axis=1, keepdims=True)
    counts = jnp.sum(cnt_ref[...], axis=1, keepdims=True)
    write_pieces(acc_ref[:, :128] + acc_ref[:, 128:], counts, local_total, out_ref)


def step_kernel(table_ref, feat_ref, virt_ref, out_ref, tab_ref, off_ref, score_ref, w_ref, acc_ref, cnt_ref):
    n = feat_ref.shape[1]
    lane = lax.broadcasted_iota(jnp.int32, (OWN, 128), 1)
    row = lax.broadcasted_iota(jnp.int32, (OWN, 128), 0)
    for m in range(MEM_SIZE):
        own = slice(m * OWN, (m + 1) * OWN)
        high, low = in_two(table_ref[m * PIECE : m * PIECE + OWN, :])
        tab_ref[own, 0:128] = high
        tab_ref[own, 128:256] = high
        tab_ref[own, 256:384] = low
        tab_ref[own, 384:512] = low
        extra = jnp.broadcast_to(table_ref[m * PIECE + OWN : (m + 1) * PIECE, :], (OWN, 128))
        for k in range(2):
            column = jnp.sum(jnp.where(lane == row + k * OWN, extra, 0.0), axis=1, keepdims=True)
            off_ref[own, k * 128 : (k + 1) * 128] = jnp.broadcast_to(column, (OWN, 128))
    for t in range(n // TILE):
        rows = slice(t * TILE, (t + 1) * TILE)
        slot = t % 2
        feats = feat_ref[:, rows]
        cross = jnp.dot(
            tab_ref[...], jnp.concatenate([feats, feats], axis=0), preferred_element_type=jnp.float32
        )
        virt = virt_ref[:, rows].astype(jnp.float32)
        for h in range(TILE // 128):
            half = slice(h * 128, (h + 1) * 128)
            score_ref[slot, :, half] = (cross[:, half] + off_ref[:, :128]) * virt[:, half] + off_ref[:, 128:]
        score = score_ref[slot]
        top = jnp.max(score, axis=0, keepdims=True)
        expd = jnp.exp2(score - top)
        ratio = virt / jnp.sum(expd, axis=0, keepdims=True)
        w = expd * ratio
        high, low = in_two(w)
        w_ref[slot, :, :TILE] = high
        w_ref[slot, :, TILE:] = low
        part = lax.dot_general(
            w_ref[slot],
            jnp.concatenate([feats, feats], axis=1),
            CONTRACT_LANES,
            preferred_element_type=jnp.float32,
        )
        add_up(t, part, w, acc_ref, cnt_ref)
    finish(virt_ref, acc_ref, cnt_ref, out_ref)


def own_parents(copies_ref):
    lane = lax.broadcasted_iota(jnp.int32, (OWN, 128), 1)
    row = lax.broadcasted_iota(jnp.int32, (OWN, 128), 0)
    sums, extra = copies_ref[:OWN, :], copies_ref[OWN:PIECE, :]
    for k in range(1, copies_ref.shape[0] // PIECE):
        sums += copies_ref[k * PIECE : k * PIECE + OWN, :]
        extra += copies_ref[k * PIECE + OWN : (k + 1) * PIECE, :]
    wide = jnp.broadcast_to(extra, (OWN, 128))
    mass = jnp.sum(jnp.where(lane == row, wide, 0.0), axis=1, keepdims=True) + 1.0
    total = wide[:, OWN : OWN + 1]
    here = jnp.where(lane < D, sums, sums + 1.0) / mass
    there = pltpu.roll(here, D, 1)
    means = jnp.where(lane < D, here, there)
    variances = jnp.where(lane < D, there, here) - means * means
    return lane, row, means, variances, mass / (total + P_SIZE)


def update_kernel(copies_ref, out_ref):
    lane, row, means, variances, weights = own_parents(copies_ref)
    scale = -0.5 / D * LOG2E
    inverse = scale / variances
    table = jnp.where(lane < D, -2.0 * means * inverse, inverse)
    terms = scale * jnp.log(2.0 * math.pi * variances) + means * means * inverse
    offset = jnp.sum(jnp.where(lane < D, terms, 0.0), axis=1, keepdims=True)
    spread = jnp.where(lane == row, offset, jnp.where(lane == row + OWN, LOG2E * jnp.log(weights), 0.0))
    extra = jnp.sum(spread, axis=0, keepdims=True)
    for m in range(MEM_SIZE):
        out_ref[m * PIECE : m * PIECE + OWN, :] = table
        out_ref[m * PIECE + OWN : (m + 1) * PIECE, :] = extra


def last_kernel(copies_ref, mean_ref, var_ref, weight_ref):
    lane, row, means, variances, weights = own_parents(copies_ref)
    mean_ref[...] = means[:, :D]
    var_ref[...] = variances[:, :D]
    weight_ref[...] = jnp.sum(jnp.where(lane == row, weights, 0.0), axis=0, keepdims=True)[:, :OWN]


def vmem(k):
    return [pl.BlockSpec(memory_space=pltpu.VMEM)] * k


def call(kernel, out_shape, scratch_shapes, name, *args, space=pltpu.VMEM, **kw):
    many = isinstance(out_shape, tuple)
    if space is pltpu.HBM:
        args = [pltpu.with_memory_space_constraint(a, space) for a in args]
    return pl.pallas_call(
        kernel,
        out_shape=out_shape,
        in_specs=[pl.BlockSpec(memory_space=space)] * len(args),
        out_specs=tuple(vmem(len(out_shape))) if many else vmem(1)[0],
        scratch_shapes=scratch_shapes,
        compiler_params=pltpu.CompilerParams(vmem_limit_bytes=20 << 20),
        name=name,
        **kw,
    )(*args)


def first_statistics(means, variances, virt, labels, **kw):
    n = means.shape[1]
    return call(
        first_kernel,
        (pltpu.VMEM((256, n), jnp.bfloat16), pltpu.VMEM((MEM_SIZE * PIECE, 128), jnp.float32)),
        [
            pltpu.VMEM((D, n), jnp.float32),
            pltpu.VMEM((D, n), jnp.float32),
            pltpu.VMEM((1, n), jnp.int32),
            pltpu.VMEM((1, n), jnp.int32),
            pltpu.VMEM((P_SIZE, 256), jnp.float32),
            pltpu.VMEM((P_SIZE, 128), jnp.float32),
            pltpu.SemaphoreType.DMA((4,)),
        ],
        "first",
        means,
        variances,
        virt,
        labels,
        space=pltpu.HBM,
        **kw,
    )


def step_statistics(table, feats, virt, **kw):
    return call(
        step_kernel,
        pltpu.VMEM((MEM_SIZE * PIECE, 128), jnp.float32),
        [
            pltpu.VMEM((P_SIZE, 512), jnp.bfloat16),
            pltpu.VMEM((P_SIZE, 256), jnp.float32),
            pltpu.VMEM((2, P_SIZE, TILE), jnp.float32),
            pltpu.VMEM((2, P_SIZE, 2 * TILE), jnp.bfloat16),
            pltpu.VMEM((P_SIZE, 256), jnp.float32),
            pltpu.VMEM((P_SIZE, 128), jnp.float32),
        ],
        "step",
        table,
        feats,
        virt,
        **kw,
    )


def reduce_own(pieces):
    size = lax.axis_size("grp")
    arrived = lax.all_to_all(pieces.reshape(MEM_SIZE, 1, PIECE * 128), MEM, 0, 0, tiled=True)
    shared = jnp.sum(arrived, axis=0, keepdims=True)
    copies = lax.all_to_all(
        jnp.broadcast_to(shared, (size, 1, PIECE * 128)), "grp", 0, 0, tiled=True
    )
    return copies.reshape(size * PIECE, 128)


def next_table(copies, **kw):
    out = call(update_kernel, pltpu.VMEM((MEM_SIZE * PIECE, 128), jnp.float32), [], "update", copies, **kw)
    gathered = lax.all_to_all(out.reshape(MEM_SIZE, 1, PIECE * 128), MEM, 0, 0, tiled=True)
    return gathered.reshape(MEM_SIZE * PIECE, 128)


def final_parents(copies, **kw):
    f32 = jnp.float32
    shapes = (
        jax.ShapeDtypeStruct((OWN, D), f32),
        jax.ShapeDtypeStruct((OWN, D), f32),
        jax.ShapeDtypeStruct((1, OWN), f32),
    )
    means, variances, weights = call(last_kernel, shapes, [], "last", copies, **kw)
    return means, variances, weights.reshape(OWN)


def shards(child_means, child_variances, virtual_counts, assignment):
    virt = virtual_counts.reshape(1, -1)
    feats, pieces = first_statistics(
        child_means.T, child_variances.T, virt, assignment.reshape(1, -1)
    )
    for iteration in range(ITERS):
        pieces = step_statistics(next_table(reduce_own(pieces)), feats, virt)
    return final_parents(reduce_own(pieces))


def solution(mesh):
    split = Mesh(
        mesh.devices.reshape(mesh.shape["grp"], 4, 4, 2), ("grp", "mem_0", "mem_1", "mem_2")
    )
    return jax.shard_map(
        shards,
        mesh=split,
        in_specs=(P(GRP_MEM, None), P(GRP_MEM, None), P(GRP_MEM), P(GRP_MEM, None)),
        out_specs=(P(MEM, None), P(MEM, None), P(MEM)),
        check_vma=False,
    )
```

```python
import math

import jax
import jax.numpy as jnp
from jax import lax
from jax.experimental import pallas as pl
from jax.experimental.pallas import tpu as pltpu
from jax.sharding import Mesh
from jax.sharding import PartitionSpec as P

D = 64
P_SIZE = 512
ITERS = 2
MEM_SIZE = 32
OWN = P_SIZE // MEM_SIZE
PIECE = OWN + 1
TILE = 256
BOTH = ("grp", "mem")
LINE = (2, 0, 1, 3)
MEM_START = 2 * 8 + 2 * 2 + 1
MEM_LIST = [8 * y + 2 * x + core for y in LINE for x in LINE for core in (0, 1)]
MEM_ORDER = MEM_LIST[MEM_LIST.index(MEM_START) :] + MEM_LIST[: MEM_LIST.index(MEM_START)]
GRP_ORDER = [4, 0, 3, 7, 2, 6, 1, 5]
LOG2E = math.log2(math.e)
CONTRACT_LANES = (((1,), (1,)), ((), ()))


def in_two(value):
    high = value.astype(jnp.bfloat16)
    return high, (value - high.astype(jnp.float32)).astype(jnp.bfloat16)


def write_pieces(sums, counts, local_total, out_ref):
    lane = lax.broadcasted_iota(jnp.int32, (OWN, 128), 1)
    row = lax.broadcasted_iota(jnp.int32, (OWN, 128), 0)
    last = lax.broadcasted_iota(jnp.int32, (1, 128), 1) == OWN
    for k, m in enumerate(MEM_ORDER):
        own = slice(m * OWN, (m + 1) * OWN)
        out_ref[k * PIECE : k * PIECE + OWN, :] = sums[own]
        spread = jnp.where(lane == row, counts[own], 0.0)
        flat = jnp.sum(spread, axis=0, keepdims=True)
        out_ref[k * PIECE + OWN : (k + 1) * PIECE, :] = jnp.where(last, local_total, flat)


def first_kernel(
    mean_hbm, var_hbm, virt_hbm, label_hbm, feat_ref, out_ref,
    mean_ref, var_ref, virt_ref, label_ref, acc_ref, cnt_ref, sem
):
    n = mean_ref.shape[1]
    copies = [
        pltpu.make_async_copy(source, target, sem.at[k])
        for k, (source, target) in enumerate(
            (
                (label_hbm, label_ref),
                (virt_hbm, virt_ref),
                (mean_hbm, mean_ref),
                (var_hbm, var_ref),
            )
        )
    ]
    for copy in copies:
        copy.start()
    for copy in copies[:2]:
        copy.wait()
    for t in range(n // TILE):
        rows = slice(t * TILE, (t + 1) * TILE)
        virt = virt_ref[:, rows].astype(jnp.float32)
        parent = lax.broadcasted_iota(jnp.int32, (P_SIZE, TILE), 0)
        w = jnp.where(parent == label_ref[:, rows], virt, 0.0)
        if t == 0:
            for copy in copies[2:]:
                copy.wait()
        mean = mean_ref[:, rows]
        high, low = in_two(jnp.concatenate([mean, var_ref[:, rows] + mean * mean], axis=0))
        feats = jnp.concatenate([high, low], axis=0)
        feat_ref[:, rows] = feats
        part = lax.dot_general(
            w.astype(jnp.bfloat16), feats, CONTRACT_LANES, preferred_element_type=jnp.float32
        )
        add_up(t, part, w, acc_ref, cnt_ref)
    finish(virt_ref, acc_ref, cnt_ref, out_ref)


def add_up(t, part, w, acc_ref, cnt_ref):
    seen = w[:, :128] + w[:, 128:]
    if t == 0:
        acc_ref[...] = part
        cnt_ref[...] = seen
    else:
        acc_ref[...] += part
        cnt_ref[...] += seen


def finish(virt_ref, acc_ref, cnt_ref, out_ref):
    local_total = jnp.sum(virt_ref[...].astype(jnp.float32), axis=1, keepdims=True)
    counts = jnp.sum(cnt_ref[...], axis=1, keepdims=True)
    write_pieces(acc_ref[:, :128] + acc_ref[:, 128:], counts, local_total, out_ref)


def step_kernel(table_ref, feat_ref, virt_ref, out_ref, tab_ref, off_ref, score_ref, w_ref, acc_ref, cnt_ref):
    n = feat_ref.shape[1]
    lane = lax.broadcasted_iota(jnp.int32, (OWN, 128), 1)
    row = lax.broadcasted_iota(jnp.int32, (OWN, 128), 0)
    for k, m in enumerate(MEM_ORDER):
        own = slice(m * OWN, (m + 1) * OWN)
        high, low = in_two(table_ref[k * PIECE : k * PIECE + OWN, :])
        tab_ref[own, 0:128] = high
        tab_ref[own, 128:256] = high
        tab_ref[own, 256:384] = low
        tab_ref[own, 384:512] = low
        extra = jnp.broadcast_to(table_ref[k * PIECE + OWN : (k + 1) * PIECE, :], (OWN, 128))
        for j in range(2):
            column = jnp.sum(jnp.where(lane == row + j * OWN, extra, 0.0), axis=1, keepdims=True)
            off_ref[own, j * 128 : (j + 1) * 128] = jnp.broadcast_to(column, (OWN, 128))
    for t in range(n // TILE):
        rows = slice(t * TILE, (t + 1) * TILE)
        slot = t % 2
        feats = feat_ref[:, rows]
        cross = jnp.dot(
            tab_ref[...], jnp.concatenate([feats, feats], axis=0), preferred_element_type=jnp.float32
        )
        virt = virt_ref[:, rows].astype(jnp.float32)
        for h in range(TILE // 128):
            half = slice(h * 128, (h + 1) * 128)
            score_ref[slot, :, half] = (cross[:, half] + off_ref[:, :128]) * virt[:, half] + off_ref[:, 128:]
        score = score_ref[slot]
        top = jnp.max(score, axis=0, keepdims=True)
        expd = jnp.exp2(score - top)
        ratio = virt / jnp.sum(expd, axis=0, keepdims=True)
        w = expd * ratio
        high, low = in_two(w)
        w_ref[slot, :, :TILE] = high
        w_ref[slot, :, TILE:] = low
        part = lax.dot_general(
            w_ref[slot],
            jnp.concatenate([feats, feats], axis=1),
            CONTRACT_LANES,
            preferred_element_type=jnp.float32,
        )
        add_up(t, part, w, acc_ref, cnt_ref)
    finish(virt_ref, acc_ref, cnt_ref, out_ref)


def own_parents(copies_ref):
    lane = lax.broadcasted_iota(jnp.int32, (OWN, 128), 1)
    row = lax.broadcasted_iota(jnp.int32, (OWN, 128), 0)
    sums, extra = copies_ref[:OWN, :], copies_ref[OWN:PIECE, :]
    for k in range(1, copies_ref.shape[0] // PIECE):
        sums += copies_ref[k * PIECE : k * PIECE + OWN, :]
        extra += copies_ref[k * PIECE + OWN : (k + 1) * PIECE, :]
    wide = jnp.broadcast_to(extra, (OWN, 128))
    mass = jnp.sum(jnp.where(lane == row, wide, 0.0), axis=1, keepdims=True) + 1.0
    total = wide[:, OWN : OWN + 1]
    here = jnp.where(lane < D, sums, sums + 1.0) / mass
    there = pltpu.roll(here, D, 1)
    means = jnp.where(lane < D, here, there)
    variances = jnp.where(lane < D, there, here) - means * means
    return lane, row, means, variances, mass / (total + P_SIZE)


def update_kernel(copies_ref, out_ref):
    lane, row, means, variances, weights = own_parents(copies_ref)
    scale = -0.5 / D * LOG2E
    inverse = scale / variances
    table = jnp.where(lane < D, -2.0 * means * inverse, inverse)
    terms = scale * jnp.log(2.0 * math.pi * variances) + means * means * inverse
    offset = jnp.sum(jnp.where(lane < D, terms, 0.0), axis=1, keepdims=True)
    spread = jnp.where(lane == row, offset, jnp.where(lane == row + OWN, LOG2E * jnp.log(weights), 0.0))
    extra = jnp.sum(spread, axis=0, keepdims=True)
    for m in range(MEM_SIZE):
        out_ref[m * PIECE : m * PIECE + OWN, :] = table
        out_ref[m * PIECE + OWN : (m + 1) * PIECE, :] = extra


def last_kernel(copies_ref, mean_ref, var_ref, weight_ref):
    lane, row, means, variances, weights = own_parents(copies_ref)
    mean_ref[...] = means[:, :D]
    var_ref[...] = variances[:, :D]
    weight_ref[...] = jnp.sum(jnp.where(lane == row, weights, 0.0), axis=0, keepdims=True)[:, :OWN]


def vmem(k):
    return [pl.BlockSpec(memory_space=pltpu.VMEM)] * k


def call(kernel, out_shape, scratch_shapes, name, *args, space=pltpu.VMEM, **kw):
    many = isinstance(out_shape, tuple)
    if space is pltpu.HBM:
        args = [pltpu.with_memory_space_constraint(a, space) for a in args]
    return pl.pallas_call(
        kernel,
        out_shape=out_shape,
        in_specs=[pl.BlockSpec(memory_space=space)] * len(args),
        out_specs=tuple(vmem(len(out_shape))) if many else vmem(1)[0],
        scratch_shapes=scratch_shapes,
        compiler_params=pltpu.CompilerParams(vmem_limit_bytes=20 << 20),
        name=name,
        **kw,
    )(*args)


def first_statistics(means, variances, virt, labels, **kw):
    n = means.shape[1]
    return call(
        first_kernel,
        (pltpu.VMEM((256, n), jnp.bfloat16), pltpu.VMEM((MEM_SIZE * PIECE, 128), jnp.float32)),
        [
            pltpu.VMEM((D, n), jnp.float32),
            pltpu.VMEM((D, n), jnp.float32),
            pltpu.VMEM((1, n), jnp.int32),
            pltpu.VMEM((1, n), jnp.int32),
            pltpu.VMEM((P_SIZE, 256), jnp.float32),
            pltpu.VMEM((P_SIZE, 128), jnp.float32),
            pltpu.SemaphoreType.DMA((4,)),
        ],
        "first",
        means,
        variances,
        virt,
        labels,
        space=pltpu.HBM,
        **kw,
    )


def step_statistics(table, feats, virt, **kw):
    return call(
        step_kernel,
        pltpu.VMEM((MEM_SIZE * PIECE, 128), jnp.float32),
        [
            pltpu.VMEM((P_SIZE, 512), jnp.bfloat16),
            pltpu.VMEM((P_SIZE, 256), jnp.float32),
            pltpu.VMEM((2, P_SIZE, TILE), jnp.float32),
            pltpu.VMEM((2, P_SIZE, 2 * TILE), jnp.bfloat16),
            pltpu.VMEM((P_SIZE, 256), jnp.float32),
            pltpu.VMEM((P_SIZE, 128), jnp.float32),
        ],
        "step",
        table,
        feats,
        virt,
        **kw,
    )


def exchange(pieces, axis, order):
    return lax.all_to_all(pieces, axis, 0, 0, axis_index_groups=[order], tiled=True)


def reduce_own(pieces):
    size = len(GRP_ORDER)
    arrived = exchange(pieces.reshape(MEM_SIZE, 1, PIECE * 128), "mem", MEM_ORDER)
    shared = jnp.sum(arrived, axis=0, keepdims=True)
    copies = exchange(jnp.broadcast_to(shared, (size, 1, PIECE * 128)), "grp", GRP_ORDER)
    return copies.reshape(size * PIECE, 128)


def next_table(copies, **kw):
    out = call(update_kernel, pltpu.VMEM((MEM_SIZE * PIECE, 128), jnp.float32), [], "update", copies, **kw)
    gathered = exchange(out.reshape(MEM_SIZE, 1, PIECE * 128), "mem", MEM_ORDER)
    return gathered.reshape(MEM_SIZE * PIECE, 128)


def final_parents(copies, **kw):
    f32 = jnp.float32
    shapes = (
        jax.ShapeDtypeStruct((OWN, D), f32),
        jax.ShapeDtypeStruct((OWN, D), f32),
        jax.ShapeDtypeStruct((1, OWN), f32),
    )
    means, variances, weights = call(last_kernel, shapes, [], "last", copies, **kw)
    return means, variances, weights.reshape(OWN)


def shards(child_means, child_variances, virtual_counts, assignment):
    virt = virtual_counts.reshape(1, -1)
    feats, pieces = first_statistics(
        child_means.T, child_variances.T, virt, assignment.reshape(1, -1)
    )
    for iteration in range(ITERS):
        pieces = step_statistics(next_table(reduce_own(pieces)), feats, virt)
    return final_parents(reduce_own(pieces))


def solution(mesh):
    return jax.shard_map(
        shards,
        mesh=mesh,
        in_specs=(P(BOTH, None), P(BOTH, None), P(BOTH), P(BOTH, None)),
        out_specs=(P("mem", None), P("mem", None), P("mem")),
        check_vma=False,
    )
```

```python
import math

import jax
import jax.numpy as jnp
from jax import lax
from jax.experimental import pallas as pl
from jax.experimental.pallas import tpu as pltpu
from jax.sharding import Mesh
from jax.sharding import PartitionSpec as P

D = 64
P_SIZE = 512
ITERS = 2
MEM_SIZE = 32
OWN = P_SIZE // MEM_SIZE
PIECE = OWN + 1
TILE = 256
BOTH = ("grp", "mem")
Y_LINE = (2, 0, 3, 1)
X_LINE = (2, 0, 1, 3)
MEM_START = 2 * 8 + 2 * 2 + 1
MEM_LIST = [8 * y + 2 * x + core for y in Y_LINE for x in X_LINE for core in (0, 1)]
MEM_ORDER = MEM_LIST[MEM_LIST.index(MEM_START) :] + MEM_LIST[: MEM_LIST.index(MEM_START)]
GRP_ORDER = [4, 0, 7, 3, 6, 2, 5, 1]
LOG2E = math.log2(math.e)
CONTRACT_LANES = (((1,), (1,)), ((), ()))


def in_two(value):
    high = value.astype(jnp.bfloat16)
    return high, (value - high.astype(jnp.float32)).astype(jnp.bfloat16)


def write_pieces(sums, counts, local_total, out_ref):
    lane = lax.broadcasted_iota(jnp.int32, (OWN, 128), 1)
    row = lax.broadcasted_iota(jnp.int32, (OWN, 128), 0)
    last = lax.broadcasted_iota(jnp.int32, (1, 128), 1) == OWN
    for k, m in enumerate(MEM_ORDER):
        own = slice(m * OWN, (m + 1) * OWN)
        out_ref[k * PIECE : k * PIECE + OWN, :] = sums[own]
        spread = jnp.where(lane == row, counts[own], 0.0)
        flat = jnp.sum(spread, axis=0, keepdims=True)
        out_ref[k * PIECE + OWN : (k + 1) * PIECE, :] = jnp.where(last, local_total, flat)


def first_kernel(
    mean_hbm, var_hbm, virt_hbm, label_hbm, feat_ref, out_ref,
    mean_ref, var_ref, virt_ref, label_ref, acc_ref, cnt_ref, sem
):
    n = mean_ref.shape[1]
    copies = [
        pltpu.make_async_copy(source, target, sem.at[k])
        for k, (source, target) in enumerate(
            (
                (label_hbm, label_ref),
                (virt_hbm, virt_ref),
                (mean_hbm, mean_ref),
                (var_hbm, var_ref),
            )
        )
    ]
    for copy in copies:
        copy.start()
    for copy in copies[:2]:
        copy.wait()
    for t in range(n // TILE):
        rows = slice(t * TILE, (t + 1) * TILE)
        virt = virt_ref[:, rows].astype(jnp.float32)
        parent = lax.broadcasted_iota(jnp.int32, (P_SIZE, TILE), 0)
        w = jnp.where(parent == label_ref[:, rows], virt, 0.0)
        if t == 0:
            for copy in copies[2:]:
                copy.wait()
        mean = mean_ref[:, rows]
        high, low = in_two(jnp.concatenate([mean, var_ref[:, rows] + mean * mean], axis=0))
        feats = jnp.concatenate([high, low], axis=0)
        feat_ref[:, rows] = feats
        part = lax.dot_general(
            w.astype(jnp.bfloat16), feats, CONTRACT_LANES, preferred_element_type=jnp.float32
        )
        add_up(t, part, w, acc_ref, cnt_ref)
    finish(virt_ref, acc_ref, cnt_ref, out_ref)


def add_up(t, part, w, acc_ref, cnt_ref):
    seen = w[:, :128] + w[:, 128:]
    if t == 0:
        acc_ref[...] = part
        cnt_ref[...] = seen
    else:
        acc_ref[...] += part
        cnt_ref[...] += seen


def finish(virt_ref, acc_ref, cnt_ref, out_ref):
    local_total = jnp.sum(virt_ref[...].astype(jnp.float32), axis=1, keepdims=True)
    counts = jnp.sum(cnt_ref[...], axis=1, keepdims=True)
    write_pieces(acc_ref[:, :128] + acc_ref[:, 128:], counts, local_total, out_ref)


def step_kernel(table_ref, feat_ref, virt_ref, out_ref, tab_ref, off_ref, score_ref, w_ref, acc_ref, cnt_ref):
    n = feat_ref.shape[1]
    lane = lax.broadcasted_iota(jnp.int32, (OWN, 128), 1)
    row = lax.broadcasted_iota(jnp.int32, (OWN, 128), 0)
    for k, m in enumerate(MEM_ORDER):
        own = slice(m * OWN, (m + 1) * OWN)
        high, low = in_two(table_ref[k * PIECE : k * PIECE + OWN, :])
        tab_ref[own, 0:128] = high
        tab_ref[own, 128:256] = high
        tab_ref[own, 256:384] = low
        tab_ref[own, 384:512] = low
        extra = jnp.broadcast_to(table_ref[k * PIECE + OWN : (k + 1) * PIECE, :], (OWN, 128))
        for j in range(2):
            column = jnp.sum(jnp.where(lane == row + j * OWN, extra, 0.0), axis=1, keepdims=True)
            off_ref[own, j * 128 : (j + 1) * 128] = jnp.broadcast_to(column, (OWN, 128))
    for t in range(n // TILE):
        rows = slice(t * TILE, (t + 1) * TILE)
        slot = t % 2
        feats = feat_ref[:, rows]
        cross = jnp.dot(
            tab_ref[...], jnp.concatenate([feats, feats], axis=0), preferred_element_type=jnp.float32
        )
        virt = virt_ref[:, rows].astype(jnp.float32)
        for h in range(TILE // 128):
            half = slice(h * 128, (h + 1) * 128)
            score_ref[slot, :, half] = (cross[:, half] + off_ref[:, :128]) * virt[:, half] + off_ref[:, 128:]
        score = score_ref[slot]
        top = jnp.max(score, axis=0, keepdims=True)
        expd = jnp.exp2(score - top)
        ratio = virt / jnp.sum(expd, axis=0, keepdims=True)
        w = expd * ratio
        high, low = in_two(w)
        w_ref[slot, :, :TILE] = high
        w_ref[slot, :, TILE:] = low
        part = lax.dot_general(
            w_ref[slot],
            jnp.concatenate([feats, feats], axis=1),
            CONTRACT_LANES,
            preferred_element_type=jnp.float32,
        )
        add_up(t, part, w, acc_ref, cnt_ref)
    finish(virt_ref, acc_ref, cnt_ref, out_ref)


def own_parents(copies_ref):
    lane = lax.broadcasted_iota(jnp.int32, (OWN, 128), 1)
    row = lax.broadcasted_iota(jnp.int32, (OWN, 128), 0)
    sums, extra = copies_ref[:OWN, :], copies_ref[OWN:PIECE, :]
    for k in range(1, copies_ref.shape[0] // PIECE):
        sums += copies_ref[k * PIECE : k * PIECE + OWN, :]
        extra += copies_ref[k * PIECE + OWN : (k + 1) * PIECE, :]
    wide = jnp.broadcast_to(extra, (OWN, 128))
    mass = jnp.sum(jnp.where(lane == row, wide, 0.0), axis=1, keepdims=True) + 1.0
    total = wide[:, OWN : OWN + 1]
    here = jnp.where(lane < D, sums, sums + 1.0) / mass
    there = pltpu.roll(here, D, 1)
    means = jnp.where(lane < D, here, there)
    variances = jnp.where(lane < D, there, here) - means * means
    return lane, row, means, variances, mass / (total + P_SIZE)


def update_kernel(copies_ref, out_ref):
    lane, row, means, variances, weights = own_parents(copies_ref)
    scale = -0.5 / D * LOG2E
    inverse = scale / variances
    table = jnp.where(lane < D, -2.0 * means * inverse, inverse)
    terms = scale * jnp.log(2.0 * math.pi * variances) + means * means * inverse
    offset = jnp.sum(jnp.where(lane < D, terms, 0.0), axis=1, keepdims=True)
    spread = jnp.where(lane == row, offset, jnp.where(lane == row + OWN, LOG2E * jnp.log(weights), 0.0))
    extra = jnp.sum(spread, axis=0, keepdims=True)
    for m in range(MEM_SIZE):
        out_ref[m * PIECE : m * PIECE + OWN, :] = table
        out_ref[m * PIECE + OWN : (m + 1) * PIECE, :] = extra


def last_kernel(copies_ref, mean_ref, var_ref, weight_ref):
    lane, row, means, variances, weights = own_parents(copies_ref)
    mean_ref[...] = means[:, :D]
    var_ref[...] = variances[:, :D]
    weight_ref[...] = jnp.sum(jnp.where(lane == row, weights, 0.0), axis=0, keepdims=True)[:, :OWN]


def vmem(k):
    return [pl.BlockSpec(memory_space=pltpu.VMEM)] * k


def call(kernel, out_shape, scratch_shapes, name, *args, space=pltpu.VMEM, **kw):
    many = isinstance(out_shape, tuple)
    if space is pltpu.HBM:
        args = [pltpu.with_memory_space_constraint(a, space) for a in args]
    return pl.pallas_call(
        kernel,
        out_shape=out_shape,
        in_specs=[pl.BlockSpec(memory_space=space)] * len(args),
        out_specs=tuple(vmem(len(out_shape))) if many else vmem(1)[0],
        scratch_shapes=scratch_shapes,
        compiler_params=pltpu.CompilerParams(vmem_limit_bytes=20 << 20),
        name=name,
        **kw,
    )(*args)


def first_statistics(means, variances, virt, labels, **kw):
    n = means.shape[1]
    return call(
        first_kernel,
        (pltpu.VMEM((256, n), jnp.bfloat16), pltpu.VMEM((MEM_SIZE * PIECE, 128), jnp.float32)),
        [
            pltpu.VMEM((D, n), jnp.float32),
            pltpu.VMEM((D, n), jnp.float32),
            pltpu.VMEM((1, n), jnp.int32),
            pltpu.VMEM((1, n), jnp.int32),
            pltpu.VMEM((P_SIZE, 256), jnp.float32),
            pltpu.VMEM((P_SIZE, 128), jnp.float32),
            pltpu.SemaphoreType.DMA((4,)),
        ],
        "first",
        means,
        variances,
        virt,
        labels,
        space=pltpu.HBM,
        **kw,
    )


def step_statistics(table, feats, virt, **kw):
    return call(
        step_kernel,
        pltpu.VMEM((MEM_SIZE * PIECE, 128), jnp.float32),
        [
            pltpu.VMEM((P_SIZE, 512), jnp.bfloat16),
            pltpu.VMEM((P_SIZE, 256), jnp.float32),
            pltpu.VMEM((2, P_SIZE, TILE), jnp.float32),
            pltpu.VMEM((2, P_SIZE, 2 * TILE), jnp.bfloat16),
            pltpu.VMEM((P_SIZE, 256), jnp.float32),
            pltpu.VMEM((P_SIZE, 128), jnp.float32),
        ],
        "step",
        table,
        feats,
        virt,
        **kw,
    )


def exchange(pieces, axis, order):
    return lax.all_to_all(pieces, axis, 0, 0, axis_index_groups=[order], tiled=True)


def reduce_own(pieces):
    size = len(GRP_ORDER)
    arrived = exchange(pieces.reshape(MEM_SIZE, 1, PIECE * 128), "mem", MEM_ORDER)
    shared = jnp.sum(arrived, axis=0, keepdims=True)
    copies = exchange(jnp.broadcast_to(shared, (size, 1, PIECE * 128)), "grp", GRP_ORDER)
    return copies.reshape(size * PIECE, 128)


def next_table(copies, **kw):
    out = call(update_kernel, pltpu.VMEM((MEM_SIZE * PIECE, 128), jnp.float32), [], "update", copies, **kw)
    gathered = exchange(out.reshape(MEM_SIZE, 1, PIECE * 128), "mem", MEM_ORDER)
    return gathered.reshape(MEM_SIZE * PIECE, 128)


def final_parents(copies, **kw):
    f32 = jnp.float32
    shapes = (
        jax.ShapeDtypeStruct((OWN, D), f32),
        jax.ShapeDtypeStruct((OWN, D), f32),
        jax.ShapeDtypeStruct((1, OWN), f32),
    )
    means, variances, weights = call(last_kernel, shapes, [], "last", copies, **kw)
    return means, variances, weights.reshape(OWN)


def shards(child_means, child_variances, virtual_counts, assignment):
    virt = virtual_counts.reshape(1, -1)
    feats, pieces = first_statistics(
        child_means.T, child_variances.T, virt, assignment.reshape(1, -1)
    )
    for iteration in range(ITERS):
        pieces = step_statistics(next_table(reduce_own(pieces)), feats, virt)
    return final_parents(reduce_own(pieces))


def solution(mesh):
    return jax.shard_map(
        shards,
        mesh=mesh,
        in_specs=(P(BOTH, None), P(BOTH, None), P(BOTH), P(BOTH, None)),
        out_specs=(P("mem", None), P("mem", None), P("mem")),
        check_vma=False,
    )
```

```python
import math

import jax
import jax.numpy as jnp
from jax import lax
from jax.experimental import pallas as pl
from jax.experimental.pallas import tpu as pltpu
from jax.sharding import Mesh
from jax.sharding import PartitionSpec as P

D = 64
P_SIZE = 512
ITERS = 2
MEM_SIZE = 32
OWN = P_SIZE // MEM_SIZE
PIECE = OWN + 1
TILE = 256
BOTH = ("grp", "mem")
Y_LINE = (2, 0, 3, 1)
X_LINE = (2, 0, 1, 3)
MEM_START = 2 * 8 + 2 * 2 + 1
MEM_LIST = [8 * y + 2 * x + core for y in Y_LINE for x in X_LINE for core in (0, 1)]
MEM_ORDER = MEM_LIST[MEM_LIST.index(MEM_START) :] + MEM_LIST[: MEM_LIST.index(MEM_START)]
GRP_ORDER = [4, 0, 7, 3, 6, 2, 5, 1]
LOG2E = math.log2(math.e)
CONTRACT_LANES = (((1,), (1,)), ((), ()))


def in_two(value):
    high = value.astype(jnp.bfloat16)
    return high, (value - high.astype(jnp.float32)).astype(jnp.bfloat16)


def write_pieces(sums, counts, local_total, out_ref):
    lane = lax.broadcasted_iota(jnp.int32, (OWN, 128), 1)
    row = lax.broadcasted_iota(jnp.int32, (OWN, 128), 0)
    last = lax.broadcasted_iota(jnp.int32, (1, 128), 1) == OWN
    for k, m in enumerate(MEM_ORDER):
        own = slice(m * OWN, (m + 1) * OWN)
        out_ref[k * PIECE : k * PIECE + OWN, :] = sums[own]
        spread = jnp.where(lane == row, counts[own], 0.0)
        flat = jnp.sum(spread, axis=0, keepdims=True)
        out_ref[k * PIECE + OWN : (k + 1) * PIECE, :] = jnp.where(last, local_total, flat)


def first_kernel(
    mean_hbm, var_hbm, virt_hbm, label_hbm, feat_ref, out_ref,
    mean_ref, var_ref, virt_ref, label_ref, acc_ref, cnt_ref, sem
):
    n = mean_ref.shape[1]
    copies = [
        pltpu.make_async_copy(source, target, sem.at[k])
        for k, (source, target) in enumerate(
            (
                (label_hbm, label_ref),
                (virt_hbm, virt_ref),
                (mean_hbm, mean_ref),
                (var_hbm, var_ref),
            )
        )
    ]
    for copy in copies:
        copy.start()
    for copy in copies[:2]:
        copy.wait()
    for t in range(n // TILE):
        rows = slice(t * TILE, (t + 1) * TILE)
        virt = virt_ref[:, rows].astype(jnp.float32)
        parent = lax.broadcasted_iota(jnp.int32, (P_SIZE, TILE), 0)
        w = jnp.where(parent == label_ref[:, rows], virt, 0.0)
        if t == 0:
            for copy in copies[2:]:
                copy.wait()
        mean = mean_ref[:, rows]
        high, low = in_two(jnp.concatenate([mean, var_ref[:, rows] + mean * mean], axis=0))
        feats = jnp.concatenate([high, low], axis=0)
        feat_ref[:, rows] = feats
        part = lax.dot_general(
            w.astype(jnp.bfloat16), feats, CONTRACT_LANES, preferred_element_type=jnp.float32
        )
        add_up(t, part, w, acc_ref, cnt_ref)
    finish(virt_ref, acc_ref, cnt_ref, out_ref)


def add_up(t, part, w, acc_ref, cnt_ref):
    seen = w[:, :128] + w[:, 128:]
    if t == 0:
        acc_ref[...] = part
        cnt_ref[...] = seen
    else:
        acc_ref[...] += part
        cnt_ref[...] += seen


def finish(virt_ref, acc_ref, cnt_ref, out_ref):
    local_total = jnp.sum(virt_ref[...].astype(jnp.float32), axis=1, keepdims=True)
    counts = jnp.sum(cnt_ref[...], axis=1, keepdims=True)
    write_pieces(acc_ref[:, :128] + acc_ref[:, 128:], counts, local_total, out_ref)


def step_kernel(table_ref, feat_ref, virt_ref, out_ref, tab_ref, off_ref, score_ref, w_ref, acc_ref, cnt_ref):
    n = feat_ref.shape[1]
    lane = lax.broadcasted_iota(jnp.int32, (OWN, 128), 1)
    row = lax.broadcasted_iota(jnp.int32, (OWN, 128), 0)
    for k, m in enumerate(MEM_ORDER):
        own = slice(m * OWN, (m + 1) * OWN)
        high, low = in_two(table_ref[k * PIECE : k * PIECE + OWN, :])
        tab_ref[own, 0:128] = high
        tab_ref[own, 128:256] = high
        tab_ref[own, 256:384] = low
        tab_ref[own, 384:512] = low
        extra = jnp.broadcast_to(table_ref[k * PIECE + OWN : (k + 1) * PIECE, :], (OWN, 128))
        for j in range(2):
            column = jnp.sum(jnp.where(lane == row + j * OWN, extra, 0.0), axis=1, keepdims=True)
            off_ref[own, j * 128 : (j + 1) * 128] = jnp.broadcast_to(column, (OWN, 128))
    for t in range(n // TILE):
        rows = slice(t * TILE, (t + 1) * TILE)
        slot = t % 2
        feats = feat_ref[:, rows]
        cross = jnp.dot(
            tab_ref[...], jnp.concatenate([feats, feats], axis=0), preferred_element_type=jnp.float32
        )
        virt = virt_ref[:, rows].astype(jnp.float32)
        for h in range(TILE // 128):
            half = slice(h * 128, (h + 1) * 128)
            score_ref[slot, :, half] = (cross[:, half] + off_ref[:, :128]) * virt[:, half] + off_ref[:, 128:]
        score = score_ref[slot]
        top = jnp.max(score, axis=0, keepdims=True)
        expd = jnp.exp2(score - top)
        ratio = virt / jnp.sum(expd, axis=0, keepdims=True)
        w = expd * ratio
        high, low = in_two(w)
        w_ref[slot, :, :TILE] = high
        w_ref[slot, :, TILE:] = low
        part = lax.dot_general(
            w_ref[slot],
            jnp.concatenate([feats, feats], axis=1),
            CONTRACT_LANES,
            preferred_element_type=jnp.float32,
        )
        add_up(t, part, w, acc_ref, cnt_ref)
    finish(virt_ref, acc_ref, cnt_ref, out_ref)


def own_parents(copies_ref):
    lane = lax.broadcasted_iota(jnp.int32, (OWN, 128), 1)
    row = lax.broadcasted_iota(jnp.int32, (OWN, 128), 0)
    sums, extra = copies_ref[:OWN, :], copies_ref[OWN:PIECE, :]
    for k in range(1, copies_ref.shape[0] // PIECE):
        sums += copies_ref[k * PIECE : k * PIECE + OWN, :]
        extra += copies_ref[k * PIECE + OWN : (k + 1) * PIECE, :]
    wide = jnp.broadcast_to(extra, (OWN, 128))
    mass = jnp.sum(jnp.where(lane == row, wide, 0.0), axis=1, keepdims=True) + 1.0
    total = wide[:, OWN : OWN + 1]
    here = jnp.where(lane < D, sums, sums + 1.0) / mass
    there = pltpu.roll(here, D, 1)
    means = jnp.where(lane < D, here, there)
    variances = jnp.where(lane < D, there, here) - means * means
    return lane, row, means, variances, mass / (total + P_SIZE)


def share_kernel(arrived_ref, out_ref):
    parts = [[], []]
    for k in range(MEM_SIZE):
        parts[0].append(arrived_ref[k * PIECE : k * PIECE + OWN, :])
        parts[1].append(arrived_ref[k * PIECE + OWN : (k + 1) * PIECE, :])
    while len(parts[0]) > 1:
        parts = [[a + b for a, b in zip(p[::2], p[1::2])] for p in parts]
    for k in range(len(GRP_ORDER)):
        out_ref[k * PIECE : k * PIECE + OWN, :] = parts[0][0]
        out_ref[k * PIECE + OWN : (k + 1) * PIECE, :] = parts[1][0]


def update_kernel(copies_ref, out_ref):
    lane, row, means, variances, weights = own_parents(copies_ref)
    scale = -0.5 / D * LOG2E
    inverse = scale / variances
    table = jnp.where(lane < D, -2.0 * means * inverse, inverse)
    terms = scale * jnp.log(2.0 * math.pi * variances) + means * means * inverse
    offset = jnp.sum(jnp.where(lane < D, terms, 0.0), axis=1, keepdims=True)
    spread = jnp.where(lane == row, offset, jnp.where(lane == row + OWN, LOG2E * jnp.log(weights), 0.0))
    extra = jnp.sum(spread, axis=0, keepdims=True)
    for m in range(MEM_SIZE):
        out_ref[m * PIECE : m * PIECE + OWN, :] = table
        out_ref[m * PIECE + OWN : (m + 1) * PIECE, :] = extra


def last_kernel(copies_ref, mean_ref, var_ref, weight_ref):
    lane, row, means, variances, weights = own_parents(copies_ref)
    mean_ref[...] = means[:, :D]
    var_ref[...] = variances[:, :D]
    weight_ref[...] = jnp.sum(jnp.where(lane == row, weights, 0.0), axis=0, keepdims=True)[:, :OWN]


def vmem(k):
    return [pl.BlockSpec(memory_space=pltpu.VMEM)] * k


def call(kernel, out_shape, scratch_shapes, name, *args, space=pltpu.VMEM, **kw):
    many = isinstance(out_shape, tuple)
    if space is pltpu.HBM:
        args = [pltpu.with_memory_space_constraint(a, space) for a in args]
    return pl.pallas_call(
        kernel,
        out_shape=out_shape,
        in_specs=[pl.BlockSpec(memory_space=space)] * len(args),
        out_specs=tuple(vmem(len(out_shape))) if many else vmem(1)[0],
        scratch_shapes=scratch_shapes,
        compiler_params=pltpu.CompilerParams(vmem_limit_bytes=20 << 20),
        name=name,
        **kw,
    )(*args)


def first_statistics(means, variances, virt, labels, **kw):
    n = means.shape[1]
    return call(
        first_kernel,
        (pltpu.VMEM((256, n), jnp.bfloat16), pltpu.VMEM((MEM_SIZE * PIECE, 128), jnp.float32)),
        [
            pltpu.VMEM((D, n), jnp.float32),
            pltpu.VMEM((D, n), jnp.float32),
            pltpu.VMEM((1, n), jnp.int32),
            pltpu.VMEM((1, n), jnp.int32),
            pltpu.VMEM((P_SIZE, 256), jnp.float32),
            pltpu.VMEM((P_SIZE, 128), jnp.float32),
            pltpu.SemaphoreType.DMA((4,)),
        ],
        "first",
        means,
        variances,
        virt,
        labels,
        space=pltpu.HBM,
        **kw,
    )


def step_statistics(table, feats, virt, **kw):
    return call(
        step_kernel,
        pltpu.VMEM((MEM_SIZE * PIECE, 128), jnp.float32),
        [
            pltpu.VMEM((P_SIZE, 512), jnp.bfloat16),
            pltpu.VMEM((P_SIZE, 256), jnp.float32),
            pltpu.VMEM((2, P_SIZE, TILE), jnp.float32),
            pltpu.VMEM((2, P_SIZE, 2 * TILE), jnp.bfloat16),
            pltpu.VMEM((P_SIZE, 256), jnp.float32),
            pltpu.VMEM((P_SIZE, 128), jnp.float32),
        ],
        "step",
        table,
        feats,
        virt,
        **kw,
    )


def exchange(pieces, axis, order):
    return lax.all_to_all(pieces, axis, 0, 0, axis_index_groups=[order], tiled=True)


def reduce_own(pieces):
    size = len(GRP_ORDER)
    arrived = exchange(pieces.reshape(MEM_SIZE, 1, PIECE * 128), "mem", MEM_ORDER)
    shared = call(
        share_kernel,
        pltpu.VMEM((size * PIECE, 128), jnp.float32),
        [],
        "share",
        arrived.reshape(MEM_SIZE * PIECE, 128),
    )
    copies = exchange(shared.reshape(size, 1, PIECE * 128), "grp", GRP_ORDER)
    return copies.reshape(size * PIECE, 128)


def next_table(copies, **kw):
    out = call(update_kernel, pltpu.VMEM((MEM_SIZE * PIECE, 128), jnp.float32), [], "update", copies, **kw)
    gathered = exchange(out.reshape(MEM_SIZE, 1, PIECE * 128), "mem", MEM_ORDER)
    return gathered.reshape(MEM_SIZE * PIECE, 128)


def final_parents(copies, **kw):
    f32 = jnp.float32
    shapes = (
        jax.ShapeDtypeStruct((OWN, D), f32),
        jax.ShapeDtypeStruct((OWN, D), f32),
        jax.ShapeDtypeStruct((1, OWN), f32),
    )
    means, variances, weights = call(last_kernel, shapes, [], "last", copies, **kw)
    return means, variances, weights.reshape(OWN)


def shards(child_means, child_variances, virtual_counts, assignment):
    virt = virtual_counts.reshape(1, -1)
    feats, pieces = first_statistics(
        child_means.T, child_variances.T, virt, assignment.reshape(1, -1)
    )
    for iteration in range(ITERS):
        pieces = step_statistics(next_table(reduce_own(pieces)), feats, virt)
    return final_parents(reduce_own(pieces))


def solution(mesh):
    return jax.shard_map(
        shards,
        mesh=mesh,
        in_specs=(P(BOTH, None), P(BOTH, None), P(BOTH), P(BOTH, None)),
        out_specs=(P("mem", None), P("mem", None), P("mem")),
        check_vma=False,
    )
```
